32 devices in a mesh: blk: 16 (over z, y, x), grp: 2 (over core).
Axes of the slice: x: 2, y: 2, z: 4, core: 2. Of those that a mesh axis runs over, the one named last changes fastest.
Arguments:
- returns: float32 [512, 8192], P(None, ('blk', 'grp')), may hold values from -200 to 200
Outputs:
- correlation: bfloat16 [8192, 8192], P(('blk', 'grp'))
The draws below stay inside these ranges and needn't reach their ends.
All inputs are finite; a program needn't handle non-finite values.
Results may differ from the reference program's by a relative error of at most 0.0034.
Values may be sent and summed in bfloat16 or wider, within the bound.
A program may use at most 128 MiB of HBM per device.

```python
import math
import jax
import jax.numpy as jnp
from jax import lax

SER_DEV = 256
BARS = 512
SERIES = 8192


def draw_returns(key, part):
    subkeys = jax.random.split(key, 4)
    factor = jnp.clip(jax.random.normal(subkeys[0], (BARS, 1), jnp.float32), -4.0, 4.0)
    position = jnp.arange(SERIES, dtype=jnp.float32)[None, :] / SERIES
    loading = 0.5 + position + 0.3 * jnp.clip(jax.random.normal(subkeys[1], (1, SERIES), jnp.float32), -4.0, 4.0)
    volatility = jnp.exp(jax.random.uniform(subkeys[2], (1, SERIES), jnp.float32, math.log(0.3), math.log(3.0)))
    specific = 0.7 * jnp.clip(jax.random.normal(subkeys[3], (BARS, SERIES), jnp.float32), -4.0, 4.0)
    return (volatility * (factor * loading + specific)).astype(jnp.float32)


def setup_inputs(seed: int = 0) -> dict:
    arg_keys = jax.random.split(jax.random.key(seed), 2)
    returns = draw_returns(jax.random.fold_in(arg_keys[1], 71), 0)
    return {"returns": returns}


def reference(returns):
    market = lax.optimization_barrier(jnp.mean(returns, axis=1, keepdims=True))
    excess = returns - market
    deviation = excess - lax.optimization_barrier(jnp.mean(excess, axis=0, keepdims=True))
    inverse = lax.rsqrt(lax.optimization_barrier(jnp.mean(deviation * deviation, axis=0, keepdims=True)) + 1e-06) / math.sqrt(BARS)
    zscores = (deviation * inverse).astype(jnp.bfloat16)
    blocks = SERIES // SER_DEV
    columns = jnp.arange(SERIES, dtype=jnp.int32) // SER_DEV

    def row_block(row_index):
        block_rows = lax.dynamic_slice_in_dim(zscores, (row_index * SER_DEV).astype(jnp.int32), SER_DEV, 1)
        products = lax.dot_general(block_rows, zscores, (((0,), (0,)), ((), ())), preferred_element_type=jnp.float32)
        return jnp.where(columns[None, :] >= row_index, products, jnp.float32(0.0)).astype(jnp.bfloat16)
    stacked = lax.map(row_block, jnp.arange(blocks, dtype=jnp.int32))
    return stacked.reshape(SERIES, SERIES)
```

```python
import functools
import math

import jax
import jax.numpy as jnp
from jax import lax
from jax.experimental import pallas as pl
from jax.experimental.pallas import tpu as pltpu
from jax.sharding import PartitionSpec as P

MESH = pl.DeviceIdType.MESH
ZC, ZX, ZY, ZD, XC, YC, D0, D1, PC = range(9)
KINDS = 12


def kernel(
    planes, r_hbm, out_hbm, r_ref, gath, zt, res, parts, sums, load_sem, out_sem, psend, precv, zsend, zrecv, send, recv
):
    bars, width = r_ref.shape
    series = width * gath.shape[0]
    blk, core = lax.axis_index("blk"), lax.axis_index("grp")
    x, y, z = lax.rem(blk, 2), lax.rem(lax.div(blk, 2), 2), lax.div(blk, 4)
    nx, ny, nc = 1 - x, 1 - y, 1 - core

    def device(zz, yy, xx, cc):
        return {"blk": (zz * 2 + yy) * 2 + xx, "grp": cc}

    def slot(zz, yy, xx, cc):
        return ((zz * 2 + yy) * 2 + xx) * 2 + cc

    mates = [
        device(z, ny if j & 2 else y, nx if j & 1 else x, nc if j & 4 else core) for j in range(1, 8)
    ]
    column = [device(lax.rem(z + d, planes), y, x, core) for d in range(1, planes)]
    barrier = pltpu.get_barrier_semaphore()
    for other in mates + column:
        pl.semaphore_signal(barrier, inc=1, device_id=other, device_id_type=MESH)
    load = pltpu.make_async_copy(r_hbm, r_ref, load_sem)
    load.start()
    load.wait()

    lanes = r_ref[:, :128]
    for i in range(1, width // 128):
        lanes = lanes + r_ref[:, 128 * i : 128 * (i + 1)]
    mine = slot(0, y, x, core)
    parts[mine] = jnp.sum(lanes.T, axis=0, keepdims=True)
    pl.semaphore_wait(barrier, len(mates) + len(column))

    def part_copy(j):
        return pltpu.make_async_remote_copy(
            parts.at[mine], parts.at[mine], psend.at[j], precv.at[j], device_id=mates[j], device_id_type=MESH
        )

    for j in range(7):
        part_copy(j).start()
    for j in range(7):
        part_copy(j).wait_recv()
    sums[z] = jnp.sum(parts[...], axis=0)

    def sum_copy(d):
        return pltpu.make_async_remote_copy(
            sums.at[z], sums.at[z], zsend.at[d], zrecv.at[d], device_id=column[d], device_id_type=MESH
        )

    for d in range(planes - 1):
        sum_copy(d).start()
    for d in range(planes - 1):
        sum_copy(d).wait_recv()
    market = jnp.sum(sums[...], axis=0) * (1.0 / series)
    market = jnp.broadcast_to(market, (128, bars)).T
    own = slot(z, y, x, core)
    for i in range(width // 128):
        excess = r_ref[:, 128 * i : 128 * (i + 1)] - market
        deviation = excess - jnp.mean(excess, axis=0, keepdims=True)
        inverse = lax.rsqrt(jnp.mean(deviation * deviation, axis=0, keepdims=True) + 1e-06) / math.sqrt(bars)
        gath[own, :, 128 * i : 128 * (i + 1)] = (deviation * inverse).astype(jnp.bfloat16)

    split = bars * 25 // 32 // 16 * 16
    half = split // 32 * 16
    whole, first, rest = (0, bars), (0, split), (split, bars - split)

    def copy(block, rows, kind, dz_send, dz_recv, target):
        ref = gath.at[block, pl.ds(*rows)]
        return pltpu.make_async_remote_copy(
            ref, ref, send.at[kind, dz_send], recv.at[kind, dz_recv], device_id=target, device_id_type=MESH
        )

    below, xdev, ydev, partner = device(z - 1, y, x, core), device(z, y, nx, core), device(z, ny, x, core), device(z, y, x, nc)

    class Step:
        def __init__(self, dz):
            self.dz = dz
            self.valid = z + dz < planes
            zz = z + dz
            here = [slot(zz, yy, xx, core) for yy, xx in ((y, x), (y, nx), (ny, x), (ny, nx))]
            there = [slot(zz, yy, xx, nc) for yy, xx in ((y, x), (y, nx), (ny, x), (ny, nx))]
            spread = whole if dz == 0 else first
            cut = bars // 2 if dz == 0 else half
            low, high = (0, cut), (cut, spread[1] - cut)
            to = functools.partial
            self.out = {
                ZC: to(copy, here[0], whole, ZC, dz, dz + 1, below),
                ZX: to(copy, here[1], rest, ZX, dz, dz + 1, below),
                ZY: to(copy, here[2], rest, ZY, dz, dz + 1, below),
                ZD: to(copy, here[3], rest, ZD, dz, dz + 1, below),
                XC: to(copy, here[0], spread, XC, dz, dz, xdev),
                YC: to(copy, here[0], spread, YC, dz, dz, ydev),
                D0: to(copy, here[1], low, D0, dz, dz, ydev),
                D1: to(copy, here[2], high, D1, dz, dz, xdev),
            }
            self.into = {
                ZC: to(copy, here[0], whole, ZC, dz, dz, below),
                ZX: to(copy, here[1], rest, ZX, dz, dz, below),
                ZY: to(copy, here[2], rest, ZY, dz, dz, below),
                ZD: to(copy, here[3], rest, ZD, dz, dz, below),
                XC: to(copy, here[1], spread, XC, dz, dz, xdev),
                YC: to(copy, here[2], spread, YC, dz, dz, ydev),
                D0: to(copy, here[3], low, D0, dz, dz, ydev),
                D1: to(copy, here[3], high, D1, dz, dz, xdev),
            }
            for i in range(4):
                self.out[PC + i] = to(copy, here[i], whole, PC + i, dz, dz, partner)
                self.into[PC + i] = to(copy, there[i], whole, PC + i, dz, dz, partner)

        def start(self, *kinds):
            for kind in kinds:
                if kind in (ZC, ZX, ZY, ZD):
                    if self.dz < planes - 1:
                        pl.when(z > 0)(lambda kind=kind: self.out[kind]().start())
                else:
                    self.out[kind]().start()

        def wait(self, *kinds):
            for kind in kinds:
                self.into[kind]().wait_recv()

        def drain(self):
            for kind, make in self.out.items():
                if kind in (ZC, ZX, ZY, ZD):
                    if self.dz < planes - 1:
                        pl.when(z > 0)(lambda make=make: make().wait_send())
                else:
                    make().wait_send()

        def spread(self):
            if self.dz > 0:
                self.wait(ZC)
            self.start(ZC, XC, YC, PC)

        def turn(self):
            self.wait(XC)
            self.start(D0)
            self.wait(YC)
            self.start(D1)
            if self.dz > 0:
                self.wait(ZX, ZY)
            self.start(ZX, ZY, PC + 1, PC + 2)
            if self.dz > 0:
                self.wait(ZD)
                self.start(ZD)

        def corner(self):
            self.wait(D0, D1)
            if self.dz == 0:
                self.start(ZD)
            self.start(PC + 3)

        def multiply(self):
            self.wait(PC, PC + 1, PC + 2, PC + 3)
            base = (z + self.dz) * 8

            @pl.loop(0, 8)
            def _(i):
                at = pl.ds(pl.multiple_of((base + i) * width, width), width)
                res[:, at] = jnp.dot(zt[...], gath[base + i], preferred_element_type=jnp.float32).astype(jnp.bfloat16)

            self.store().start()

        def store(self):
            at = pl.ds(pl.multiple_of((z + self.dz) * 8 * width, 8 * width), 8 * width)
            return pltpu.make_async_copy(res.at[:, at], out_hbm.at[:, at], out_sem.at[self.dz])

    steps = [Step(dz) for dz in range(planes)]

    def stage(dz, name):
        if 0 <= dz < planes:
            if dz == 0:
                getattr(steps[dz], name)()
            else:
                pl.when(steps[dz].valid)(getattr(steps[dz], name))

    for t in range(planes + 3):
        stage(t, "spread")
        if t == 0:
            zt[...] = gath[own].T
        stage(t - 1, "turn")
        stage(t - 2, "corner")
        stage(t - 3, "multiply")
    for j in range(7):
        part_copy(j).wait_send()
    for d in range(planes - 1):
        sum_copy(d).wait_send()
    for dz in range(planes):
        stage(dz, "drain")
        pl.when(steps[dz].valid)(lambda dz=dz: steps[dz].store().wait())


def shards(planes, returns):
    bars, width = returns.shape
    blocks = planes * 8
    products = pl.pallas_call(
        functools.partial(kernel, planes),
        out_shape=jax.ShapeDtypeStruct((width, blocks * width), jnp.bfloat16),
        in_specs=[pl.BlockSpec(memory_space=pl.ANY)],
        out_specs=pl.BlockSpec(memory_space=pl.ANY),
        scratch_shapes=[
            pltpu.VMEM((bars, width), jnp.float32),
            pltpu.VMEM((blocks, bars, width), jnp.bfloat16),
            pltpu.VMEM((width, bars), jnp.bfloat16),
            pltpu.VMEM((width, blocks * width), jnp.bfloat16),
            pltpu.VMEM((8, 1, bars), jnp.float32),
            pltpu.VMEM((planes, 1, bars), jnp.float32),
            pltpu.SemaphoreType.DMA,
            pltpu.SemaphoreType.DMA((planes,)),
            pltpu.SemaphoreType.DMA((7,)),
            pltpu.SemaphoreType.DMA((7,)),
            pltpu.SemaphoreType.DMA((max(planes - 1, 1),)),
            pltpu.SemaphoreType.DMA((max(planes - 1, 1),)),
            pltpu.SemaphoreType.DMA((KINDS, planes)),
            pltpu.SemaphoreType.DMA((KINDS, planes)),
        ],
        compiler_params=pltpu.CompilerParams(collective_id=0, has_side_effects=True),
    )(returns)
    my_index = lax.axis_index(("blk", "grp"))
    column_block = jnp.arange(blocks * width, dtype=jnp.int32) // width
    return jnp.where(column_block[None, :] >= my_index, products, jnp.bfloat16(0.0))


def solution(mesh):
    planes = mesh.shape["blk"] // 4
    in_specs = (P(None, ("blk", "grp")),)
    out_specs = P(("blk", "grp"), None)
    return jax.shard_map(
        functools.partial(shards, planes), mesh=mesh, in_specs=in_specs, out_specs=out_specs, check_vma=False
    )
```

```python
import functools
import math

import jax
import jax.numpy as jnp
from jax import lax
from jax.experimental import pallas as pl
from jax.experimental.pallas import tpu as pltpu
from jax.sharding import PartitionSpec as P

MESH = pl.DeviceIdType.MESH
DOWN = ("ZA", "ZB", "ZO", "ZX", "ZY", "ZD")
SPREAD = ("XA", "XB", "YA", "YB", "D0", "D1")
REST = ("XR", "YR")
PARTNER = ("P0", "P1", "P2", "P3")
KINDS = DOWN + SPREAD + REST + PARTNER
WAITS = {
    "ZA": -0.99, "ZB": -0.69, "ZO": 1.78, "ZX": 1.11, "ZY": 0.89, "ZD": 2.22, "XA": 0.73, "XB": 1.51,
    "YA": 1.22, "YB": 0.52, "XR": 1.64, "YR": 0.76, "D0": 2.25, "D1": 2.77, "M0": 2.85, "M1": 3.16,
}
SENDS = (
    "D1", "XA", "ZA", "P3", "ZD", "YB", "XR", "ZB", "ZX", "D0", "ZY", "P0", "ZO", "YR", "P2", "YA", "P1", "XB",
)


def needs(kind, d):
    first = d == 0
    return {
        "ZA": [] if first else ["ZA"],
        "ZB": [] if first else ["ZB"],
        "ZO": [] if first else ["ZO"],
        "ZX": ["XR"] if first else ["ZX"],
        "ZY": ["YR"] if first else ["ZY"],
        "ZD": ["D1"] if first else ["ZD"],
        "XA": [] if first else ["ZA"],
        "YA": [] if first else ["ZA"],
        "XB": [] if first else ["ZB"],
        "YB": [] if first else ["ZB"],
        "XR": [],
        "YR": [],
        "D0": ["XA"],
        "D1": ["YB", "YR"] if first else ["YB"],
        "P0": [] if first else ["ZA", "ZB", "ZO"],
        "P1": ["XA", "XB", "XR" if first else "ZX"],
        "P2": ["YA", "YB", "YR" if first else "ZY"],
        "P3": ["D0", "D1"] if first else ["D0", "D1", "ZD"],
    }[kind]


def sends_down(action, kind, d):
    return kind in DOWN and action in ("start", "drain")


def plan(planes):
    events = []
    for d in range(planes):
        kinds = SPREAD + (DOWN if d else REST) + ("M0", "M1")
        events += [(d + WAITS[kind], kind, d) for kind in kinds]
    here, sent, actions = set(), set(), []

    def send():
        for d in range(planes):
            for kind in SENDS:
                absent = (kind in REST and d > 0) or (kind in DOWN and d == planes - 1)
                if (kind, d) not in sent and not absent and all((k, d) in here for k in needs(kind, d)):
                    sent.add((kind, d))
                    actions.append(("start", kind, d))

    send()
    for _, kind, d in sorted(events):
        if kind in ("M0", "M1"):
            actions.extend(("wait", k, d) for k in (PARTNER[:3] if kind == "M0" else PARTNER[3:]))
            actions.append(("multiply", kind, d))
        else:
            actions.append(("wait", kind, d))
            here.add((kind, d))
            send()
    return actions


def kernel(
    planes, r_hbm, out_ref, r_ref, gath, zt, parts, sums, load_sem, psend, precv, zsend, zrecv, send, recv
):
    bars, width = r_ref.shape
    series = width * gath.shape[0]
    blk, core = lax.axis_index("blk"), lax.axis_index("grp")
    x, y, z = lax.rem(blk, 2), lax.rem(lax.div(blk, 2), 2), lax.div(blk, 4)
    nx, ny, nc = 1 - x, 1 - y, 1 - core

    def device(zz, yy, xx, cc):
        return {"blk": (zz * 2 + yy) * 2 + xx, "grp": cc}

    def slot(zz, yy, xx, cc):
        return ((zz * 2 + yy) * 2 + xx) * 2 + cc

    mates = [
        device(z, ny if j & 2 else y, nx if j & 1 else x, nc if j & 4 else core) for j in range(1, 8)
    ]
    column = [device(lax.rem(z + d, planes), y, x, core) for d in range(1, planes)]
    barrier = pltpu.get_barrier_semaphore()
    for other in mates + column:
        pl.semaphore_signal(barrier, inc=1, device_id=other, device_id_type=MESH)
    load = pltpu.make_async_copy(r_hbm, r_ref, load_sem)
    load.start()
    load.wait()

    lanes = r_ref[:, :128]
    for i in range(1, width // 128):
        lanes = lanes + r_ref[:, 128 * i : 128 * (i + 1)]
    mine = slot(0, y, x, core)
    parts[mine] = jnp.sum(lanes.T, axis=0, keepdims=True)
    pl.semaphore_wait(barrier, len(mates) + len(column))

    def part_copy(j):
        return pltpu.make_async_remote_copy(
            parts.at[mine], parts.at[mine], psend.at[j], precv.at[j], device_id=mates[j], device_id_type=MESH
        )

    for j in range(7):
        part_copy(j).start()
    for j in range(7):
        part_copy(j).wait_recv()
    sums[z] = jnp.sum(parts[...], axis=0)

    def sum_copy(d):
        return pltpu.make_async_remote_copy(
            sums.at[z], sums.at[z], zsend.at[d], zrecv.at[d], device_id=column[d], device_id_type=MESH
        )

    for d in range(planes - 1):
        sum_copy(d).start()
    for d in range(planes - 1):
        sum_copy(d).wait_recv()
    market = jnp.sum(sums[...], axis=0) * (1.0 / series)
    market = jnp.broadcast_to(market, (128, bars)).T
    own = slot(z, y, x, core)
    for i in range(width // 128):
        excess = r_ref[:, 128 * i : 128 * (i + 1)] - market
        deviation = excess - jnp.mean(excess, axis=0, keepdims=True)
        inverse = lax.rsqrt(jnp.mean(deviation * deviation, axis=0, keepdims=True) + 1e-06) / math.sqrt(bars)
        gath[own, :, 128 * i : 128 * (i + 1)] = (deviation * inverse).astype(jnp.bfloat16)

    high = bars * 25 // 32 // 16 * 16
    half = bars * 13 // 32 // 16 * 16
    rows_a, rows_b, rows_r = (0, half), (half, high - half), (high, bars - high)

    def copy(kind, d, arriving):
        zz = z + d
        link = kind[0] if kind[0] != "D" else ("Y" if kind == "D0" else "X")
        down = link == "Z"
        if arriving:
            flip = {"X": (0, 1), "Y": (1, 0), "D": (1, 1)}.get(kind[0], (0, 0))
        else:
            flip = {"D0": (0, 1), "D1": (1, 0)}.get(kind, (0, 0))
        if down:
            flip = {"ZX": (0, 1), "ZY": (1, 0), "ZD": (1, 1)}.get(kind, (0, 0))
            rows = {"ZA": rows_a, "ZB": rows_b}.get(kind, rows_r)
        elif link == "P":
            flip = {"P0": (0, 0), "P1": (0, 1), "P2": (1, 0), "P3": (1, 1)}[kind]
            rows = (0, bars)
        else:
            last = (half, bars - half) if d == 0 else rows_b
            rows = {"A": rows_a, "B": rows_b, "R": rows_r, "0": rows_a, "1": last}[kind[1]]
        owner = nc if link == "P" and arriving else core
        block = slot(zz, ny if flip[0] else y, nx if flip[1] else x, owner)
        target = {
            "Z": device(z - 1, y, x, core),
            "X": device(z, y, nx, core),
            "Y": device(z, ny, x, core),
            "P": device(z, y, x, nc),
        }[link]
        ref, k = gath.at[block, pl.ds(*rows)], KINDS.index(kind)
        return pltpu.make_async_remote_copy(
            ref,
            ref,
            send.at[k, d],
            recv.at[k, d + 1 if down and not arriving else d],
            device_id=target,
            device_id_type=MESH,
        )

    def multiply(kind, d):
        base, count = (0, 6) if kind == "M0" else (6, 2)

        @pl.loop(0, count)
        def _(i):
            chip, other = lax.div(i + base, 2), lax.rem(i, 2)
            flip_x, flip_y = lax.rem(chip, 2), lax.div(chip, 2)
            block = slot(z + d, y + flip_y * (1 - 2 * y), x + flip_x * (1 - 2 * x), other)
            at = pl.ds(pl.multiple_of(block * width, width), width)
            out_ref[:, at] = jnp.dot(zt[...], gath[block], preferred_element_type=jnp.float32).astype(jnp.bfloat16)

    def act(action, kind, d):
        if action == "multiply":
            multiply(kind, d)
        elif action == "wait":
            copy(kind, d, True).wait_recv()
        else:
            end = copy(kind, d, False)
            (end.start if action == "start" else end.wait_send)()

    actions = plan(planes)
    actions += [("drain", kind, d) for action, kind, d in actions if action == "start"]
    transposed = False
    while actions:
        key = (actions[0][2], sends_down(*actions[0]))
        count = 1
        while count < len(actions) and (actions[count][2], sends_down(*actions[count])) == key:
            count += 1
        batch, actions = actions[:count], actions[count:]

        def run(batch=batch):
            for action in batch:
                act(*action)

        if not transposed and batch[0][0] != "start":
            zt[...] = gath[own].T
            transposed = True
        d, down = key
        if down:
            pl.when(jnp.minimum(z, planes - z - d) > 0)(run)
        elif d:
            pl.when(z + d < planes)(run)
        else:
            run()
    for j in range(7):
        part_copy(j).wait_send()
    for d in range(planes - 1):
        sum_copy(d).wait_send()


def shards(planes, returns):
    bars, width = returns.shape
    blocks = planes * 8
    held = blocks * width * (2 * bars + 2 * width) + 6 * bars * width
    products = pl.pallas_call(
        functools.partial(kernel, planes),
        out_shape=jax.ShapeDtypeStruct((width, blocks * width), jnp.bfloat16),
        in_specs=[pl.BlockSpec(memory_space=pltpu.HBM)],
        out_specs=pl.BlockSpec(memory_space=pltpu.VMEM),
        scratch_shapes=[
            pltpu.VMEM((bars, width), jnp.float32),
            pltpu.VMEM((blocks, bars, width), jnp.bfloat16),
            pltpu.VMEM((width, bars), jnp.bfloat16),
            pltpu.VMEM((8, 1, bars), jnp.float32),
            pltpu.VMEM((planes, 1, bars), jnp.float32),
            pltpu.SemaphoreType.DMA,
            pltpu.SemaphoreType.DMA((7,)),
            pltpu.SemaphoreType.DMA((7,)),
            pltpu.SemaphoreType.DMA((max(planes - 1, 1),)),
            pltpu.SemaphoreType.DMA((max(planes - 1, 1),)),
            pltpu.SemaphoreType.DMA((len(KINDS), planes)),
            pltpu.SemaphoreType.DMA((len(KINDS), planes)),
        ],
        compiler_params=pltpu.CompilerParams(
            collective_id=0, has_side_effects=True, vmem_limit_bytes=held + 4 * 1024 * 1024
        ),
    )(returns)
    my_index = lax.axis_index(("blk", "grp"))
    column_block = jnp.arange(blocks * width, dtype=jnp.int32) // width
    return jnp.where(column_block[None, :] >= my_index, products, jnp.bfloat16(0.0))


def solution(mesh):
    planes = mesh.shape["blk"] // 4
    in_specs = (P(None, ("blk", "grp")),)
    out_specs = P(("blk", "grp"), None)
    return jax.shard_map(
        functools.partial(shards, planes), mesh=mesh, in_specs=in_specs, out_specs=out_specs, check_vma=False
    )
```

```python
import functools
import math

import jax
import jax.numpy as jnp
from jax import lax
from jax.experimental import pallas as pl
from jax.experimental.pallas import tpu as pltpu
from jax.sharding import PartitionSpec as P

MESH = pl.DeviceIdType.MESH
DOWN = ("ZA", "ZB", "ZO", "ZX", "ZY", "ZD")
SPREAD = ("XA", "XB", "YA", "YB", "D0", "D1")
REST = ("XR", "YR")
PARTNER = ("P0", "P1", "P2", "P3", "P4")
KINDS = DOWN + SPREAD + REST + PARTNER
WAITS = {
    "ZA": -0.99, "ZB": -0.69, "ZO": 1.78, "ZX": 1.11, "ZY": 0.89, "ZD": 2.22, "XA": 0.73, "XB": 1.51,
    "YA": 1.22, "YB": 0.52, "XR": 1.64, "YR": 0.76, "D0": 2.25, "D1": 2.77, "M0": 2.85, "M1": 3.16,
}
SENDS = (
    "D1", "XA", "ZA", "P3", "P4", "ZD", "YB", "XR", "ZB", "ZX", "D0", "ZY", "P0", "ZO", "YR", "P2", "YA", "P1", "XB",
)


def needs(kind, d):
    first = d == 0
    return {
        "ZA": [] if first else ["ZA"],
        "ZB": [] if first else ["ZB"],
        "ZO": [] if first else ["ZO"],
        "ZX": ["XR"] if first else ["ZX"],
        "ZY": ["YR"] if first else ["ZY"],
        "ZD": ["D1"] if first else ["ZD"],
        "XA": [] if first else ["ZA"],
        "YA": [] if first else ["ZA"],
        "XB": [] if first else ["ZB"],
        "YB": [] if first else ["ZB"],
        "XR": [],
        "YR": [],
        "D0": ["XA"],
        "D1": ["YB", "YR"] if first else ["YB"],
        "P0": [] if first else ["ZA", "ZB", "ZO"],
        "P1": ["XA", "XB", "XR" if first else "ZX"],
        "P2": ["YA", "YB", "YR" if first else "ZY"],
        "P3": ["D0"],
        "P4": ["D1"] if first else ["D1", "ZD"],
    }[kind]


def sends_down(action, kind, d):
    return kind in DOWN and action in ("start", "drain")


def plan(planes):
    events = []
    for d in range(planes):
        kinds = SPREAD + (DOWN if d else REST) + ("M0", "M1")
        events += [(d + WAITS[kind], kind, d) for kind in kinds]
    here, sent, actions = set(), set(), []

    def send():
        for d in range(planes):
            for kind in SENDS:
                absent = (kind in REST and d > 0) or (kind in DOWN and d == planes - 1)
                if (kind, d) not in sent and not absent and all((k, d) in here for k in needs(kind, d)):
                    sent.add((kind, d))
                    actions.append(("start", kind, d))

    send()
    for _, kind, d in sorted(events):
        if kind in ("M0", "M1"):
            actions.extend(("wait", k, d) for k in (PARTNER[:3] if kind == "M0" else PARTNER[3:]))
            actions.append(("multiply", kind, d))
        else:
            actions.append(("wait", kind, d))
            here.add((kind, d))
            send()
    return actions


def kernel(
    planes, r_hbm, out_ref, r_ref, gath, zt, parts, sums, load_sem, psend, precv, zsend, zrecv, send, recv
):
    bars, width = r_ref.shape
    series = width * gath.shape[0]
    blk, core = lax.axis_index("blk"), lax.axis_index("grp")
    x, y, z = lax.rem(blk, 2), lax.rem(lax.div(blk, 2), 2), lax.div(blk, 4)
    nx, ny, nc = 1 - x, 1 - y, 1 - core

    def device(zz, yy, xx, cc):
        return {"blk": (zz * 2 + yy) * 2 + xx, "grp": cc}

    def slot(zz, yy, xx, cc):
        return ((zz * 2 + yy) * 2 + xx) * 2 + cc

    mates = [
        device(z, ny if j & 2 else y, nx if j & 1 else x, nc if j & 4 else core) for j in range(1, 8)
    ]
    column = [device(lax.rem(z + d, planes), y, x, core) for d in range(1, planes)]
    barrier = pltpu.get_barrier_semaphore()
    for other in mates + column:
        pl.semaphore_signal(barrier, inc=1, device_id=other, device_id_type=MESH)
    load = pltpu.make_async_copy(r_hbm, r_ref, load_sem)
    load.start()
    load.wait()

    lanes = r_ref[:, :128]
    for i in range(1, width // 128):
        lanes = lanes + r_ref[:, 128 * i : 128 * (i + 1)]
    mine = slot(0, y, x, core)
    parts[mine] = jnp.sum(lanes.T, axis=0, keepdims=True)
    pl.semaphore_wait(barrier, len(mates) + len(column))

    def part_copy(j):
        return pltpu.make_async_remote_copy(
            parts.at[mine], parts.at[mine], psend.at[j], precv.at[j], device_id=mates[j], device_id_type=MESH
        )

    for j in range(7):
        part_copy(j).start()
    for j in range(7):
        part_copy(j).wait_recv()
    sums[z] = jnp.sum(parts[...], axis=0)

    def sum_copy(d):
        return pltpu.make_async_remote_copy(
            sums.at[z], sums.at[z], zsend.at[d], zrecv.at[d], device_id=column[d], device_id_type=MESH
        )

    for d in range(planes - 1):
        sum_copy(d).start()
    for d in range(planes - 1):
        sum_copy(d).wait_recv()
    market = jnp.sum(sums[...], axis=0) * (1.0 / series)
    market = jnp.broadcast_to(market, (128, bars)).T
    own = slot(z, y, x, core)
    for i in range(width // 128):
        excess = r_ref[:, 128 * i : 128 * (i + 1)] - market
        deviation = excess - jnp.mean(excess, axis=0, keepdims=True)
        inverse = lax.rsqrt(jnp.mean(deviation * deviation, axis=0, keepdims=True) + 1e-06) / math.sqrt(bars)
        gath[own, :, 128 * i : 128 * (i + 1)] = (deviation * inverse).astype(jnp.bfloat16)

    high = bars * 25 // 32 // 16 * 16
    half = bars * 13 // 32 // 16 * 16
    rows_a, rows_b, rows_r = (0, half), (half, high - half), (high, bars - high)

    def copy(kind, d, arriving):
        zz = z + d
        link = kind[0] if kind[0] != "D" else ("Y" if kind == "D0" else "X")
        down = link == "Z"
        if arriving:
            flip = {"X": (0, 1), "Y": (1, 0), "D": (1, 1)}.get(kind[0], (0, 0))
        else:
            flip = {"D0": (0, 1), "D1": (1, 0)}.get(kind, (0, 0))
        if down:
            flip = {"ZX": (0, 1), "ZY": (1, 0), "ZD": (1, 1)}.get(kind, (0, 0))
            rows = {"ZA": rows_a, "ZB": rows_b}.get(kind, rows_r)
        elif link == "P":
            flip = {"P0": (0, 0), "P1": (0, 1), "P2": (1, 0)}.get(kind, (1, 1))
            rows = {"P3": rows_a, "P4": (half, bars - half)}.get(kind, (0, bars))
        else:
            last = (half, bars - half) if d == 0 else rows_b
            rows = {"A": rows_a, "B": rows_b, "R": rows_r, "0": rows_a, "1": last}[kind[1]]
        owner = nc if link == "P" and arriving else core
        block = slot(zz, ny if flip[0] else y, nx if flip[1] else x, owner)
        target = {
            "Z": device(z - 1, y, x, core),
            "X": device(z, y, nx, core),
            "Y": device(z, ny, x, core),
            "P": device(z, y, x, nc),
        }[link]
        ref, k = gath.at[block, pl.ds(*rows)], KINDS.index(kind)
        return pltpu.make_async_remote_copy(
            ref,
            ref,
            send.at[k, d],
            recv.at[k, d + 1 if down and not arriving else d],
            device_id=target,
            device_id_type=MESH,
        )

    def multiply(kind, d):
        base, count = (0, 6) if kind == "M0" else (6, 2)

        @pl.loop(0, count)
        def _(i):
            chip, other = lax.div(i + base, 2), lax.rem(i, 2)
            flip_x, flip_y = lax.rem(chip, 2), lax.div(chip, 2)
            block = slot(z + d, y + flip_y * (1 - 2 * y), x + flip_x * (1 - 2 * x), other)
            at = pl.ds(pl.multiple_of(block * width, width), width)
            out_ref[:, at] = jnp.dot(zt[...], gath[block], preferred_element_type=jnp.float32).astype(jnp.bfloat16)

    def act(action, kind, d):
        if action == "multiply":
            multiply(kind, d)
        elif action == "wait":
            copy(kind, d, True).wait_recv()
        else:
            end = copy(kind, d, False)
            (end.start if action == "start" else end.wait_send)()

    actions = plan(planes)
    actions += [("drain", kind, d) for action, kind, d in actions if action == "start"]
    transposed = False
    while actions:
        key = (actions[0][2], sends_down(*actions[0]))
        count = 1
        while count < len(actions) and (actions[count][2], sends_down(*actions[count])) == key:
            count += 1
        batch, actions = actions[:count], actions[count:]

        def run(batch=batch):
            for action in batch:
                act(*action)

        if not transposed and batch[0][0] != "start":
            zt[...] = gath[own].T
            transposed = True
        d, down = key
        if down:
            pl.when(jnp.minimum(z, planes - z - d) > 0)(run)
        elif d:
            pl.when(z + d < planes)(run)
        else:
            run()
    for j in range(7):
        part_copy(j).wait_send()
    for d in range(planes - 1):
        sum_copy(d).wait_send()


def shards(planes, returns):
    bars, width = returns.shape
    blocks = planes * 8
    held = blocks * width * (2 * bars + 2 * width) + 6 * bars * width
    products = pl.pallas_call(
        functools.partial(kernel, planes),
        out_shape=jax.ShapeDtypeStruct((width, blocks * width), jnp.bfloat16),
        in_specs=[pl.BlockSpec(memory_space=pltpu.HBM)],
        out_specs=pl.BlockSpec(memory_space=pltpu.VMEM),
        scratch_shapes=[
            pltpu.VMEM((bars, width), jnp.float32),
            pltpu.VMEM((blocks, bars, width), jnp.bfloat16),
            pltpu.VMEM((width, bars), jnp.bfloat16),
            pltpu.VMEM((8, 1, bars), jnp.float32),
            pltpu.VMEM((planes, 1, bars), jnp.float32),
            pltpu.SemaphoreType.DMA,
            pltpu.SemaphoreType.DMA((7,)),
            pltpu.SemaphoreType.DMA((7,)),
            pltpu.SemaphoreType.DMA((max(planes - 1, 1),)),
            pltpu.SemaphoreType.DMA((max(planes - 1, 1),)),
            pltpu.SemaphoreType.DMA((len(KINDS), planes)),
            pltpu.SemaphoreType.DMA((len(KINDS), planes)),
        ],
        compiler_params=pltpu.CompilerParams(
            collective_id=0, has_side_effects=True, vmem_limit_bytes=held + 4 * 1024 * 1024
        ),
    )(pltpu.with_memory_space_constraint(returns, pltpu.HBM))
    my_index = lax.axis_index(("blk", "grp"))
    column_block = jnp.arange(blocks * width, dtype=jnp.int32) // width
    return jnp.where(column_block[None, :] >= my_index, products, jnp.bfloat16(0.0))


def solution(mesh):
    planes = mesh.shape["blk"] // 4
    in_specs = (P(None, ("blk", "grp")),)
    out_specs = P(("blk", "grp"), None)
    return jax.shard_map(
        functools.partial(shards, planes), mesh=mesh, in_specs=in_specs, out_specs=out_specs, check_vma=False
    )
```

```python
import functools
import math

import jax
import jax.numpy as jnp
from jax import lax
from jax.experimental import pallas as pl
from jax.experimental.pallas import tpu as pltpu
from jax.sharding import PartitionSpec as P

MESH = pl.DeviceIdType.MESH
DOWN = ("ZA", "ZB", "ZO", "ZX", "ZY", "ZD")
SPREAD = ("XA", "XB", "YA", "YB", "D0", "D1")
REST = ("XR", "YR")
PARTNER = ("P0", "P1", "P2", "P3", "P4")
PRODUCTS = ("M0", "M1", "M2", "M3")
KINDS = DOWN + SPREAD + REST + PARTNER
WAITS = {
    "ZA": -0.08,
    "ZB": 0.26,
    "ZO": 1.1,
    "ZX": 2.33,
    "ZY": 1.62,
    "ZD": 2.78,
    "XA": 1.26,
    "XB": 2.64,
    "YA": 1.39,
    "YB": 1.22,
    "XR": 1.54,
    "YR": 0.39,
    "D0": 2.83,
    "D1": 2.89,
    "M0": 1.43,
    "M1": 3.2,
    "M2": 2.03,
    "M3": 3.72,
}
SENDS = (
    "D1", "XA", "YR", "P1", "ZA", "P2", "ZB", "ZX", "P3", "P4", "YB", "XR", "XB", "D0", "ZO", "ZD", "ZY", "P0", "YA",
)


def needs(kind, d):
    first = d == 0
    return {
        "ZA": [] if first else ["ZA"],
        "ZB": [] if first else ["ZB"],
        "ZO": [] if first else ["ZO"],
        "ZX": ["XR"] if first else ["ZX"],
        "ZY": ["YR"] if first else ["ZY"],
        "ZD": ["D1"] if first else ["ZD"],
        "XA": [] if first else ["ZA"],
        "YA": [] if first else ["ZA"],
        "XB": [] if first else ["ZB"],
        "YB": [] if first else ["ZB"],
        "XR": [],
        "YR": [],
        "D0": ["XA"],
        "D1": ["YB", "YR"] if first else ["YB"],
        "P0": [] if first else ["ZA", "ZB", "ZO"],
        "P1": ["XA", "XB", "XR" if first else "ZX"],
        "P2": ["YA", "YB", "YR" if first else "ZY"],
        "P3": ["D0"],
        "P4": ["D1"] if first else ["D1", "ZD"],
    }[kind]


def sends_down(action, kind, d):
    return kind in DOWN and action in ("start", "drain")


def plan(planes):
    events = []
    for d in range(planes):
        kinds = SPREAD + (DOWN if d else REST) + PRODUCTS
        events += [(d + WAITS[kind], kind, d) for kind in kinds]
    here, sent, actions = set(), set(), []

    def send():
        for d in range(planes):
            for kind in SENDS:
                absent = (kind in REST and d > 0) or (kind in DOWN and d == planes - 1)
                if (kind, d) not in sent and not absent and all((k, d) in here for k in needs(kind, d)):
                    sent.add((kind, d))
                    actions.append(("start", kind, d))

    send()
    for _, kind, d in sorted(events):
        if kind in PRODUCTS:
            actions.extend(("wait", k, d) for k in (PARTNER[3:] if kind == "M3" else ("P" + kind[1],)))
            actions.append(("multiply", kind, d))
        else:
            actions.append(("wait", kind, d))
            here.add((kind, d))
            send()
    return actions


def kernel(
    planes, r_hbm, out_ref, r_ref, gath, zt, parts, sums, load_sem, psend, precv, zsend, zrecv, send, recv
):
    bars, width = r_ref.shape
    series = width * gath.shape[0]
    blk, core = lax.axis_index("blk"), lax.axis_index("grp")
    x, y, z = lax.rem(blk, 2), lax.rem(lax.div(blk, 2), 2), lax.div(blk, 4)
    nx, ny, nc = 1 - x, 1 - y, 1 - core

    def device(zz, yy, xx, cc):
        return {"blk": (zz * 2 + yy) * 2 + xx, "grp": cc}

    def slot(zz, yy, xx, cc):
        return ((zz * 2 + yy) * 2 + xx) * 2 + cc

    mates = [
        device(z, ny if j & 2 else y, nx if j & 1 else x, nc if j & 4 else core) for j in range(1, 8)
    ]
    column = [device(lax.rem(z + d, planes), y, x, core) for d in range(1, planes)]
    barrier = pltpu.get_barrier_semaphore()
    for other in mates + column:
        pl.semaphore_signal(barrier, inc=1, device_id=other, device_id_type=MESH)
    load = pltpu.make_async_copy(r_hbm, r_ref, load_sem)
    load.start()
    load.wait()

    lanes = r_ref[:, :128]
    for i in range(1, width // 128):
        lanes = lanes + r_ref[:, 128 * i : 128 * (i + 1)]
    mine = slot(0, y, x, core)
    parts[mine] = jnp.sum(lanes.T, axis=0, keepdims=True)
    pl.semaphore_wait(barrier, len(mates) + len(column))

    def part_copy(j):
        return pltpu.make_async_remote_copy(
            parts.at[mine], parts.at[mine], psend.at[j], precv.at[j], device_id=mates[j], device_id_type=MESH
        )

    for j in range(7):
        part_copy(j).start()
    for j in range(7):
        part_copy(j).wait_recv()
    sums[z] = jnp.sum(parts[...], axis=0)

    def sum_copy(d):
        return pltpu.make_async_remote_copy(
            sums.at[z], sums.at[z], zsend.at[d], zrecv.at[d], device_id=column[d], device_id_type=MESH
        )

    for d in range(planes - 1):
        sum_copy(d).start()
    for d in range(planes - 1):
        sum_copy(d).wait_recv()
    market = jnp.sum(sums[...], axis=0) * (1.0 / series)
    market = jnp.broadcast_to(market, (128, bars)).T
    own = slot(z, y, x, core)
    for i in range(width // 128):
        excess = r_ref[:, 128 * i : 128 * (i + 1)] - market
        deviation = excess - jnp.mean(excess, axis=0, keepdims=True)
        inverse = lax.rsqrt(jnp.mean(deviation * deviation, axis=0, keepdims=True) + 1e-06) / math.sqrt(bars)
        gath[own, :, 128 * i : 128 * (i + 1)] = (deviation * inverse).astype(jnp.bfloat16)

    high = bars * 25 // 32 // 16 * 16
    half = bars * 13 // 32 // 16 * 16
    rows_a, rows_b, rows_r = (0, half), (half, high - half), (high, bars - high)

    def copy(kind, d, arriving):
        zz = z + d
        link = kind[0] if kind[0] != "D" else ("Y" if kind == "D0" else "X")
        down = link == "Z"
        if arriving:
            flip = {"X": (0, 1), "Y": (1, 0), "D": (1, 1)}.get(kind[0], (0, 0))
        else:
            flip = {"D0": (0, 1), "D1": (1, 0)}.get(kind, (0, 0))
        if down:
            flip = {"ZX": (0, 1), "ZY": (1, 0), "ZD": (1, 1)}.get(kind, (0, 0))
            rows = {"ZA": rows_a, "ZB": rows_b}.get(kind, rows_r)
        elif link == "P":
            flip = {"P0": (0, 0), "P1": (0, 1), "P2": (1, 0)}.get(kind, (1, 1))
            rows = {"P3": rows_a, "P4": (half, bars - half)}.get(kind, (0, bars))
        else:
            last = (half, bars - half) if d == 0 else rows_b
            rows = {"A": rows_a, "B": rows_b, "R": rows_r, "0": rows_a, "1": last}[kind[1]]
        owner = nc if link == "P" and arriving else core
        block = slot(zz, ny if flip[0] else y, nx if flip[1] else x, owner)
        target = {
            "Z": device(z - 1, y, x, core),
            "X": device(z, y, nx, core),
            "Y": device(z, ny, x, core),
            "P": device(z, y, x, nc),
        }[link]
        ref, k = gath.at[block, pl.ds(*rows)], KINDS.index(kind)
        return pltpu.make_async_remote_copy(
            ref,
            ref,
            send.at[k, d],
            recv.at[k, d + 1 if down and not arriving else d],
            device_id=target,
            device_id_type=MESH,
        )

    def multiply(kind, d):
        far_y, far_x = divmod(int(kind[1]), 2)

        @pl.loop(0, 2)
        def _(other):
            block = slot(z + d, ny if far_y else y, nx if far_x else x, other)
            at = pl.ds(pl.multiple_of(block * width, width), width)
            out_ref[:, at] = jnp.dot(zt[...], gath[block], preferred_element_type=jnp.float32).astype(jnp.bfloat16)

    def act(action, kind, d):
        if action == "multiply":
            multiply(kind, d)
        elif action == "wait":
            copy(kind, d, True).wait_recv()
        else:
            end = copy(kind, d, False)
            (end.start if action == "start" else end.wait_send)()

    actions = plan(planes)
    actions += [("drain", kind, d) for action, kind, d in actions if action == "start"]
    transposed = False
    while actions:
        key = (actions[0][2], sends_down(*actions[0]))
        count = 1
        while count < len(actions) and (actions[count][2], sends_down(*actions[count])) == key:
            count += 1
        batch, actions = actions[:count], actions[count:]

        def run(batch=batch):
            for action in batch:
                act(*action)

        if not transposed and batch[0][0] != "start":
            zt[...] = gath[own].T
            transposed = True
        d, down = key
        if down:
            pl.when(jnp.minimum(z, planes - z - d) > 0)(run)
        elif d:
            pl.when(z + d < planes)(run)
        else:
            run()
    for j in range(7):
        part_copy(j).wait_send()
    for d in range(planes - 1):
        sum_copy(d).wait_send()


def shards(planes, returns):
    bars, width = returns.shape
    blocks = planes * 8
    held = blocks * width * (2 * bars + 2 * width) + 6 * bars * width
    products = pl.pallas_call(
        functools.partial(kernel, planes),
        out_shape=jax.ShapeDtypeStruct((width, blocks * width), jnp.bfloat16),
        in_specs=[pl.BlockSpec(memory_space=pltpu.HBM)],
        out_specs=pl.BlockSpec(memory_space=pltpu.VMEM),
        scratch_shapes=[
            pltpu.VMEM((bars, width), jnp.float32),
            pltpu.VMEM((blocks, bars, width), jnp.bfloat16),
            pltpu.VMEM((width, bars), jnp.bfloat16),
            pltpu.VMEM((8, 1, bars), jnp.float32),
            pltpu.VMEM((planes, 1, bars), jnp.float32),
            pltpu.SemaphoreType.DMA,
            pltpu.SemaphoreType.DMA((7,)),
            pltpu.SemaphoreType.DMA((7,)),
            pltpu.SemaphoreType.DMA((max(planes - 1, 1),)),
            pltpu.SemaphoreType.DMA((max(planes - 1, 1),)),
            pltpu.SemaphoreType.DMA((len(KINDS), planes)),
            pltpu.SemaphoreType.DMA((len(KINDS), planes)),
        ],
        compiler_params=pltpu.CompilerParams(
            collective_id=0, has_side_effects=True, vmem_limit_bytes=held + 4 * 1024 * 1024
        ),
    )(pltpu.with_memory_space_constraint(returns, pltpu.HBM))
    my_index = lax.axis_index(("blk", "grp"))
    column_block = jnp.arange(blocks * width, dtype=jnp.int32) // width
    return jnp.where(column_block[None, :] >= my_index, products, jnp.bfloat16(0.0))


def solution(mesh):
    planes = mesh.shape["blk"] // 4
    in_specs = (P(None, ("blk", "grp")),)
    out_specs = P(("blk", "grp"), None)
    return jax.shard_map(
        functools.partial(shards, planes), mesh=mesh, in_specs=in_specs, out_specs=out_specs, check_vma=False
    )
```
